256 devices in a mesh: trial: 2 (over core), qa: 16 (over y, x), qb: 8 (over z).
Axes of the slice: x: 4, y: 4, z: 8, core: 2. Of those that a mesh axis runs over, the one named last changes fastest.
Arguments:
- wave_parts: float32 [4, 512, 128, 128], P('trial', ('qa', 'qb')), parts along dimension 0, may hold values from -6 to 6
- level_table: float32 [1024, 128, 128], P(('trial', 'qa', 'qb')), parts along dimension 0, may hold values from -2 to 2
- diagonal_angles: float32 [6, 128], P('trial'), parts along dimension 0, may hold values from 0.3 to 1.2
- turn_angles: float32 [6, 4], P('trial'), parts along dimension 0, may hold values from 0.3 to 1.2
Outputs:
- final_parts: float32 [4, 512, 128, 128], P('trial', ('qa', 'qb')), parts along dimension 0
The draws below stay inside these ranges and needn't reach their ends.
There are 2 independent parts, one for each index of `trial`. The reference program is written for one: setup_inputs(seed, part) draws one part's arguments, and reference() takes and returns one part's arrays. A program takes and returns all parts, laid end to end along the dimension named above; each array names one. Nothing has to cross between parts.
All inputs are finite; a program needn't handle non-finite values.
Results may differ from the reference program's by a relative error of at most 0.0003.
Values sent between devices are 32-bit elements.
A program may use at most 64 MiB of HBM per device.

```python
import jax
import jax.numpy as jnp
from jax import lax

BLOCKS_DEV = 4
ROWS = 128
LANES = 128
BLOCKS = 512
LAYERS = 3
N_QA = 16
N_QB = 8


def block_scale(own_key, dims, pieces, smallest, high):
    def one(position, blocks):
        heights = jax.random.uniform(jax.random.fold_in(jax.random.fold_in(own_key, 6), position), (blocks,), jnp.float32, smallest / len(pieces), high / len(pieces))
        return jnp.repeat(jnp.exp(heights), dims[position] // blocks).reshape((-1,) + (1,) * (len(dims) - position - 1))

    factor_of = one(*pieces[0])
    for cut in pieces[1:]:
        factor_of = factor_of * one(*cut)
    return factor_of


def scatter_about(rng, dims, spread, most, cuts=(), kind=jnp.bfloat16):
    values = spread * jax.random.normal(rng, dims, jnp.float32)
    if cuts:
        values = values * block_scale(rng, dims, cuts, -0.22, 0.18)
    return jnp.clip(values, -most, most).astype(kind)


def setup_inputs(seed: int = 0, part: int = 0) -> dict:
    key_of = jax.random.split(jax.random.key(seed), 5)
    own_keys = jax.random.split(jax.random.fold_in(key_of[4], part), 5)
    wave_parts = scatter_about(own_keys[0], (2, BLOCKS, ROWS, LANES), 1.0, 6.0, ((1, 128),), jnp.float32)
    level_table = jnp.clip(jax.random.uniform(own_keys[1], (BLOCKS, ROWS, LANES), jnp.float32, -2.0, 2.0) * block_scale(own_keys[1], (BLOCKS, ROWS, LANES), ((0, 128),), -0.4, 0.0), -2.0, 2.0)
    diagonal_angles = jnp.clip(jax.random.uniform(own_keys[2], (LAYERS, LANES), jnp.float32, 0.3, 1.2), 0.3, 1.2)
    turn_angles = jnp.clip(jax.random.uniform(own_keys[3], (LAYERS, 4), jnp.float32, 0.3, 1.2), 0.3, 1.2)
    return dict(wave_parts=wave_parts, level_table=level_table, diagonal_angles=diagonal_angles, turn_angles=turn_angles)


def count_bits(values, count):
    places = jnp.arange(count.bit_length() - 1, dtype=jnp.int32)
    return jnp.sum((values[..., None] >> places) & 1, axis=-1)


def rotation_table(count, angle):
    rank = jnp.arange(count, dtype=jnp.int32)
    apart = count_bits(rank[:, None] ^ rank[None, :], count)
    bits = count.bit_length() - 1
    size = jnp.cos(angle) ** (bits - apart).astype(jnp.float32) * jnp.sin(angle) ** apart.astype(jnp.float32)
    real_sign = jnp.where(apart % 4 == 0, 1.0, jnp.where(apart % 4 == 2, -1.0, 0.0)).astype(jnp.float32)
    imag_sign = jnp.where(apart % 4 == 1, -1.0, jnp.where(apart % 4 == 3, 1.0, 0.0)).astype(jnp.float32)
    return size * real_sign, size * imag_sign


def mix_dim(values, dim, angle):
    real_part, imag_part = rotation_table(values.shape[dim], angle)
    def times(table):
        moved = jnp.tensordot(values, table, axes=([dim], [0]), precision=lax.Precision.HIGHEST)
        return jnp.moveaxis(moved, -1, dim)
    by_real = times(real_part)
    by_imag = times(imag_part)
    return jnp.stack([by_real[0] - by_imag[1], by_real[1] + by_imag[0]])


def phase_step(values, levels, angle):
    turn = angle * levels
    return jnp.stack([values[0] * jnp.cos(turn) + values[1] * jnp.sin(turn), values[1] * jnp.cos(turn) - values[0] * jnp.sin(turn)])


def reference(wave_parts, level_table, diagonal_angles, turn_angles):
    values = wave_parts
    for layer in range(LAYERS):
        values = phase_step(values, level_table, diagonal_angles[layer])
        values = mix_dim(values, 3, turn_angles[layer, 0])
        values = mix_dim(values, 2, turn_angles[layer, 1])
        parts = values.reshape(2, N_QA, N_QB, BLOCKS_DEV, ROWS, LANES)
        parts = mix_dim(parts, 1, turn_angles[layer, 2])
        parts = mix_dim(parts, 2, turn_angles[layer, 3])
        parts = mix_dim(parts, 3, turn_angles[layer, 2])
        values = parts.reshape(values.shape)
    return values
```

```python
import functools

import jax
import jax.numpy as jnp
from jax import lax
from jax.experimental import pallas as pl
from jax.experimental.pallas import tpu as pltpu
from jax.sharding import PartitionSpec as P

LAYERS = 3
LANE, ROW, OUTER, MIDDLE = range(4)


def log2(count):
    return count.bit_length() - 1


def cos_sin(turn):
    half = 0.5 * turn
    y = half * half
    sine = -1 / 39916800
    for term in (1 / 362880, -1 / 5040, 1 / 120, -1 / 6, 1.0):
        sine = sine * y + term
    sine = sine * half
    cosine = 1 / 479001600
    for term in (-1 / 3628800, 1 / 40320, -1 / 720, 1 / 24, -0.5, 1.0):
        cosine = cosine * y + term
    return 1.0 - 2.0 * sine * sine, 2.0 * sine * cosine


def split(x):
    high = x.astype(jnp.bfloat16)
    return high, (x - high.astype(jnp.float32)).astype(jnp.bfloat16)


def dot(a, b, dims):
    return lax.dot_general(a, b, (dims, ((), ())), preferred_element_type=jnp.float32)


def right_weights(table):
    high, low = split(table)
    return jnp.concatenate(
        [jnp.concatenate([high, low], 1), jnp.concatenate([high, jnp.zeros_like(low)], 1)], 0)


def left_weights(table):
    high, low = split(table)
    return jnp.concatenate(
        [jnp.concatenate([high, high], 1), jnp.concatenate([low, jnp.zeros_like(low)], 1)], 0)


def times_right(x, weights):
    both = dot(jnp.concatenate(split(x), 1), weights, ((1,), (0,)))
    size = both.shape[1] // 2
    return both[:, :size] + both[:, size:]


def times_left(weights, x):
    both = dot(weights, jnp.concatenate(split(x), 0), ((1,), (0,)))
    size = both.shape[0] // 2
    return both[:size] + both[size:]


def times_left_turned(weights, x):
    both = dot(weights, jnp.concatenate(split(x), 1), ((1,), (1,)))
    size = both.shape[0] // 2
    return both[:size] + both[size:]


def turn_table(size, turns):
    out = lax.broadcasted_iota(jnp.int32, (8, size), 0)
    into = lax.broadcasted_iota(jnp.int32, (8, size), 1)
    table = None
    for i in range(3):
        c, s = turns[i]
        o, t = out >> i & 1, into >> i & 1
        factor = jnp.where(o == t, c, jnp.where(o > t, -s, s))
        table = factor if table is None else table * factor
    for i in range(3, log2(size)):
        c, s = turns[i]
        t = (into >> i & 1) == 0
        table = jnp.concatenate([_times(table, jnp.where(t, c, s)), _times(table, jnp.where(t, -s, c))], 0)
    return table


def _times(table, factor):
    rows = [table[i : i + 8] * factor for i in range(0, table.shape[0], 8)]
    return rows[0] if len(rows) == 1 else jnp.concatenate(rows, 0)


def mix_pair(u, v, turn):
    c, s = turn
    return c * u + s * v, c * v - s * u


def kernel(na, nb, wave_hbm, level_hbm, diag_hbm, turns_hbm, out, wave, level, diag, turns, in_sem,
           st, rt, s1, r1, s2, r2, s3, r3, cs, half, tables, send_sem, recv_sem):
    n = na * nb
    f32 = jnp.float32
    a = lax.axis_index("qa")
    b = lax.axis_index("qb")
    me = a * nb + b

    def peer_of(k):
        pa = lax.rem(a + lax.div(k, nb), na)
        pb = lax.rem(b + lax.rem(k, nb), nb)
        return pa * nb + pb, {"qa": pa, "qb": pb}

    fetched = [
        pltpu.make_async_copy(src, dst, in_sem.at[i])
        for i, (src, dst) in enumerate(
            ((turns_hbm, turns), (level_hbm, level), (diag_hbm, diag), (wave_hbm, wave)))
    ]
    for copy in fetched:
        copy.start()

    barrier = pltpu.get_barrier_semaphore()

    def greet(k, carry):
        pl.semaphore_signal(barrier, inc=1, device_id=peer_of(k)[1], device_id_type=pl.DeviceIdType.MESH)
        return carry

    lax.fori_loop(1, n, greet, 0)

    def tile(ref, i, part):
        first, count = part
        return ref.at[pl.ds(pl.multiple_of(i * 8, 8) + first, count)]

    def send(src, dst, which, part):
        def step(k, carry):
            peer, to = peer_of(k)
            pltpu.make_async_remote_copy(
                src_ref=tile(src, peer, part), dst_ref=tile(dst, me, part), send_sem=send_sem.at[which],
                recv_sem=recv_sem.at[which], device_id=to, device_id_type=pl.DeviceIdType.MESH).start()
            return carry

        lax.fori_loop(1, n, step, 0)
        first, count = part
        dst[pl.ds(pl.multiple_of(me * 8, 8), 8), :] = src[pl.ds(pl.multiple_of(me * 8, 8), 8), :]

    def total(ref, sem, part):
        whole = ref.at[pl.ds(0, (n - 1) * part[1])]
        return pltpu.make_async_copy(whole, whole, sem)

    def arrive(dst, which, part):
        total(dst, recv_sem.at[which], part).wait()

    def sent(src, which, part):
        total(src, send_sem.at[which], part).wait()

    FULL, LOW, HIGH = (0, 8), (0, 4), (4, 4)

    def plane(j):
        return pl.ds(j, n, stride=8)

    fetched[0].wait()
    angle = [[cos_sin(jnp.full((1, n), turns[layer, g], f32)) for g in range(4)] for layer in range(LAYERS)]
    bits = log2(n)

    def lane_turns(layer):
        return [angle[layer][LANE]] * bits

    def row_turns(layer):
        return [angle[layer][ROW]] * bits

    def device_turns(layer):
        return [angle[layer][MIDDLE]] * log2(nb) + [angle[layer][OUTER]] * log2(na)

    def back(turn_list):
        return [(c, -s) for c, s in turn_list]

    tables[0] = right_weights(turn_table(n, back(lane_turns(0))))
    tables[1] = left_weights(turn_table(n, row_turns(0)))

    pop = jnp.zeros((8, n), jnp.int32)
    row8 = lax.broadcasted_iota(jnp.int32, (8, n), 0)
    lane8 = lax.broadcasted_iota(jnp.int32, (8, n), 1)
    for i in range(3):
        pop = pop + (row8 >> i & 1)
    for i in range(bits):
        pop = pop + (lane8 >> i & 1) + lax.rem(lax.div(me, 1 << i), 2)
    pop = pop & 3
    fr = jnp.where(pop == 0, 1.0, jnp.where(pop == 2, -1.0, 0.0))
    fi = jnp.where(pop == 1, -1.0, jnp.where(pop == 3, 1.0, 0.0))
    quarter = [(fr, fi), (fi, -fr), (-fr, -fi), (-fi, fr)]

    def power(block):
        picks = [quarter[(v.bit_count() + block.bit_count()) % 4] for v in range(n // 8)]
        return [jnp.concatenate([p[i] for p in picks], 0) if len(picks) > 1 else picks[0][i] for i in range(2)]

    fetched[1].wait()
    for g in range(4):
        st[plane(g), :] = level[g]
    pl.semaphore_wait(barrier, n - 1)
    send(st, rt, 0, LOW)

    fetched[2].wait()
    fetched[3].wait()
    planes = [[], []]
    for g in range(4):
        c, s = cos_sin(diag[0:1, :] * level[g])
        re, im = wave[0, g], wave[1, g]
        re, im = re * c + im * s, im * c - re * s
        pr, pi = power(g)
        planes[0].append(re * pr - im * pi)
        planes[1].append(im * pr + re * pi)

    def mix_blocks(xs, turn):
        xs[0], xs[2] = mix_pair(xs[0], xs[2], turn)
        xs[1], xs[3] = mix_pair(xs[1], xs[3], turn)
        xs[0], xs[1] = mix_pair(xs[0], xs[1], turn)
        xs[2], xs[3] = mix_pair(xs[2], xs[3], turn)
        return xs

    def columns(x):
        return [x[:, i : i + n] for i in range(0, x.shape[1], n)]

    for p in range(2):
        x = times_right(jnp.concatenate(planes[p], 0), tables[0])
        x = jnp.concatenate([x[g * n : (g + 1) * n] for g in range(4)], 1)
        x = times_left(tables[1], x)
        for g, x in enumerate(mix_blocks(columns(x), angle[0][OUTER])):
            s1[plane(p * 4 + g), :] = x
    send(s1, r1, 1, FULL)

    for g in range(4):
        st[plane(4 + g), :] = level[g].T
    send(st, rt, 2, HIGH)

    tables[2] = left_weights(turn_table(n, device_turns(0)))
    tables[3] = left_weights(turn_table(n, device_turns(1)))
    tables[4] = left_weights(turn_table(n, lane_turns(1)))

    arrive(rt, 0, LOW)
    for g in range(4):
        c, s = cos_sin(diag[1:2, :] * rt[plane(g), :])
        cs[0, g] = c
        cs[1, g] = s

    arrive(r1, 1, FULL)
    for p in range(2):
        x = jnp.concatenate([r1[plane(p * 4 + g), :] for g in range(4)], 1)
        x = times_left(tables[2], x)
        for g, x in enumerate(columns(x)):
            half[p, g] = x
    turned = [[], []]
    for g in range(4):
        re, im = half[0, g], half[1, g]
        c, s = cs[0, g], cs[1, g]
        turned[0].append(re * c + im * s)
        turned[1].append(im * c - re * s)
    for p in range(2):
        x = times_left(tables[3], jnp.concatenate(turned[p], 1))
        x = times_left_turned(tables[4], jnp.concatenate(columns(x), 0))
        for g, x in enumerate(mix_blocks(columns(x), angle[1][OUTER])):
            s2[plane((g % 2) * 4 + p * 2 + g // 2), :] = x
    send(s2, r2, 3, LOW)
    send(s2, r2, 4, HIGH)

    tables[5] = left_weights(turn_table(n, row_turns(1)))
    tables[6] = left_weights(turn_table(n, row_turns(2)))
    tables[7] = left_weights(turn_table(n, device_turns(2)))
    tables[8] = left_weights(turn_table(n, lane_turns(2)))

    lane1 = lax.broadcasted_iota(jnp.int32, (1, n), 1)
    own = jnp.sum(jnp.where(lane1 == me, diag[2:3, :], 0.0), axis=1, keepdims=True)
    arrive(rt, 2, HIGH)
    for g in range(4):
        c, s = cos_sin(own * rt[plane(4 + g), :].T)
        cs[0, g] = c
        cs[1, g] = s

    for q, part in enumerate((LOW, HIGH)):
        arrive(r2, 3 + q, part)
        pair = []
        for p in range(2):
            x = jnp.concatenate([r2[plane(q * 4 + p * 2 + g), :] for g in range(2)], 1)
            pair.append(columns(times_left(tables[5], x)))
        turned = [[], []]
        for g in range(2):
            re, im = pair[0][g], pair[1][g]
            c, s = cs[0, g * 2 + q], cs[1, g * 2 + q]
            turned[0].append(re * c + im * s)
            turned[1].append(im * c - re * s)
        for p in range(2):
            x = times_left(tables[6], jnp.concatenate(turned[p], 1))
            x = times_left_turned(tables[7], jnp.concatenate(columns(x), 0))
            for g, x in enumerate(mix_pair(*columns(x), angle[2][OUTER])):
                s3[plane(q * 4 + p * 2 + g), :] = x
        send(s3, r3, 5 + q, part)

    for q, part in enumerate((LOW, HIGH)):
        arrive(r3, 5 + q, part)
        for p in range(2):
            x = jnp.concatenate([r3[plane(q * 4 + p * 2 + g), :] for g in range(2)], 1)
            for g, x in enumerate(columns(times_left(tables[8], x))):
                half[p, g * 2 + q] = x.T
    for h in range(2):
        pairs = [mix_pair(half[p, h * 2], half[p, h * 2 + 1], angle[2][OUTER]) for p in range(2)]
        for q in range(2):
            re, im = pairs[0][q], pairs[1][q]
            pr, pi = power(h * 2 + q)
            out[0, h * 2 + q] = re * pr + im * pi
            out[1, h * 2 + q] = im * pr - re * pi

    sent(st, 0, LOW)
    sent(s1, 1, FULL)
    sent(st, 2, HIGH)
    for q, part in enumerate((LOW, HIGH)):
        sent(s2, 3 + q, part)
        sent(s3, 5 + q, part)


def fused(wave_parts, level_table, diagonal_angles, turn_angles, na, nb):
    n = na * nb
    f32 = jnp.float32
    V = pltpu.VMEM
    tiles = V((n * 8, n), f32)
    return pl.pallas_call(
        functools.partial(kernel, na, nb),
        out_shape=jax.ShapeDtypeStruct(wave_parts.shape, f32),
        in_specs=[pl.BlockSpec(memory_space=pltpu.HBM)] * 4,
        out_specs=pl.BlockSpec(memory_space=pltpu.VMEM),
        scratch_shapes=[
            V(wave_parts.shape, f32), V(level_table.shape, f32), V(diagonal_angles.shape, f32),
            pltpu.SMEM(turn_angles.shape, f32), pltpu.SemaphoreType.DMA((4,)),
            tiles, tiles, tiles, tiles, tiles, tiles, tiles, tiles,
            V((2,) + level_table.shape, f32), V(wave_parts.shape, f32),
            V((9, 2 * n, 2 * n), jnp.bfloat16),
            pltpu.SemaphoreType.DMA((7,)), pltpu.SemaphoreType.DMA((7,)),
        ],
        compiler_params=pltpu.CompilerParams(
            collective_id=0, has_side_effects=True, vmem_limit_bytes=32 * 1024 * 1024),
    )(wave_parts, level_table, diagonal_angles, turn_angles)


def solution(mesh):
    na, nb = mesh.shape["qa"], mesh.shape["qb"]

    def each(wave_parts, level_table, diagonal_angles, turn_angles):
        return fused(wave_parts, level_table, diagonal_angles, turn_angles, na, nb)

    placed = (
        P("trial", ("qa", "qb"), None, None),
        P(("trial", "qa", "qb"), None, None),
        P("trial", None),
        P("trial", None),
    )
    return jax.shard_map(
        each,
        mesh=mesh,
        in_specs=placed,
        out_specs=P("trial", ("qa", "qb"), None, None),
        check_vma=False,
    )
```

```python
import functools

import jax
import jax.numpy as jnp
from jax import lax
from jax.experimental import pallas as pl
from jax.experimental.pallas import tpu as pltpu
from jax.sharding import PartitionSpec as P

LAYERS = 3
LANE, ROW, OUTER, MIDDLE = range(4)


def log2(count):
    return count.bit_length() - 1


def cos_sin(turn):
    half = 0.5 * turn
    y = half * half
    sine = -1 / 39916800
    for term in (1 / 362880, -1 / 5040, 1 / 120, -1 / 6, 1.0):
        sine = sine * y + term
    sine = sine * half
    cosine = 1 / 479001600
    for term in (-1 / 3628800, 1 / 40320, -1 / 720, 1 / 24, -0.5, 1.0):
        cosine = cosine * y + term
    return 1.0 - 2.0 * sine * sine, 2.0 * sine * cosine


def split(x):
    high = x.astype(jnp.bfloat16)
    return high, (x - high.astype(jnp.float32)).astype(jnp.bfloat16)


def dot(a, b, dims):
    return lax.dot_general(a, b, (dims, ((), ())), preferred_element_type=jnp.float32)


def right_weights(table):
    high, low = split(table)
    return jnp.concatenate(
        [jnp.concatenate([high, low], 1), jnp.concatenate([high, jnp.zeros_like(low)], 1)], 0)


def left_weights(table):
    high, low = split(table)
    return jnp.concatenate(
        [jnp.concatenate([high, high], 1), jnp.concatenate([low, jnp.zeros_like(low)], 1)], 0)


def times_right(x, weights):
    both = dot(jnp.concatenate(split(x), 1), weights, ((1,), (0,)))
    size = both.shape[1] // 2
    return both[:, :size] + both[:, size:]


def times_left(weights, x):
    both = dot(weights, jnp.concatenate(split(x), 0), ((1,), (0,)))
    size = both.shape[0] // 2
    return both[:size] + both[size:]


def times_left_turned(weights, x):
    both = dot(weights, jnp.concatenate(split(x), 1), ((1,), (1,)))
    size = both.shape[0] // 2
    return both[:size] + both[size:]


def turn_table(size, turns):
    out = lax.broadcasted_iota(jnp.int32, (8, size), 0)
    into = lax.broadcasted_iota(jnp.int32, (8, size), 1)
    table = None
    for i in range(3):
        c, s = turns[i]
        o, t = out >> i & 1, into >> i & 1
        factor = jnp.where(o == t, c, jnp.where(o > t, -s, s))
        table = factor if table is None else table * factor
    for i in range(3, log2(size)):
        c, s = turns[i]
        t = (into >> i & 1) == 0
        table = jnp.concatenate([_times(table, jnp.where(t, c, s)), _times(table, jnp.where(t, -s, c))], 0)
    return table


def _times(table, factor):
    rows = [table[i : i + 8] * factor for i in range(0, table.shape[0], 8)]
    return rows[0] if len(rows) == 1 else jnp.concatenate(rows, 0)


def mix_pair(u, v, turn):
    c, s = turn
    return c * u + s * v, c * v - s * u


def kernel(na, nb, wave_hbm, level_hbm, diag_hbm, turns_hbm, out, wave, level, diag, turns, in_sem,
           st, rt, s1, r1, s2, r2, s3, r3, cs, half, tables, send_sem, recv_sem):
    n = na * nb
    f32 = jnp.float32
    a = lax.axis_index("qa")
    b = lax.axis_index("qb")
    me = a * nb + b

    places = [lax.rem(b + j, nb) for j in range(nb)]
    away = sorted(range(1, nb), key=lambda j: -min(j, nb - j))

    def each_peer(visit):
        def step(i, carry, shifts):
            pa = lax.rem(a + i, na)
            for j in shifts:
                visit(pa * nb + places[j], {"qa": pa, "qb": places[j]})
            return carry

        step(0, 0, away)
        lax.fori_loop(1, na, functools.partial(step, shifts=[0] + away), 0)

    fetched = [
        pltpu.make_async_copy(src, dst, in_sem.at[i])
        for i, (src, dst) in enumerate(
            ((turns_hbm, turns), (level_hbm, level), (diag_hbm, diag), (wave_hbm, wave)))
    ]
    for copy in fetched:
        copy.start()

    barrier = pltpu.get_barrier_semaphore()

    def greet(peer, to):
        pl.semaphore_signal(barrier, inc=1, device_id=to, device_id_type=pl.DeviceIdType.MESH)

    each_peer(greet)

    def tile(ref, i, part):
        first, count = part
        return ref.at[pl.ds(pl.multiple_of(i * 8, 8) + first, count)]

    def send(src, dst, which, part):
        def visit(peer, to):
            pltpu.make_async_remote_copy(
                src_ref=tile(src, peer, part), dst_ref=tile(dst, me, part), send_sem=send_sem.at[which],
                recv_sem=recv_sem.at[which], device_id=to, device_id_type=pl.DeviceIdType.MESH).start()

        each_peer(visit)
        own = pl.ds(pl.multiple_of(me * 8, 8), 8)
        dst[own, :] = src[own, :]

    def total(ref, sem, part):
        whole = ref.at[pl.ds(0, (n - 1) * part[1])]
        return pltpu.make_async_copy(whole, whole, sem)

    def arrive(dst, which, part):
        total(dst, recv_sem.at[which], part).wait()

    def sent(src, which, part):
        total(src, send_sem.at[which], part).wait()

    FULL, LOW, HIGH = (0, 8), (0, 4), (4, 4)

    def plane(j):
        return pl.ds(j, n, stride=8)

    fetched[0].wait()
    angle = [[cos_sin(jnp.full((1, n), turns[layer, g], f32)) for g in range(4)] for layer in range(LAYERS)]
    bits = log2(n)

    def lane_turns(layer):
        return [angle[layer][LANE]] * bits

    def row_turns(layer):
        return [angle[layer][ROW]] * bits

    def device_turns(layer):
        return [angle[layer][MIDDLE]] * log2(nb) + [angle[layer][OUTER]] * log2(na)

    def back(turn_list):
        return [(c, -s) for c, s in turn_list]

    tables[0] = right_weights(turn_table(n, back(lane_turns(0))))
    tables[1] = left_weights(turn_table(n, row_turns(0)))

    pop = jnp.zeros((8, n), jnp.int32)
    row8 = lax.broadcasted_iota(jnp.int32, (8, n), 0)
    lane8 = lax.broadcasted_iota(jnp.int32, (8, n), 1)
    for i in range(3):
        pop = pop + (row8 >> i & 1)
    for i in range(bits):
        pop = pop + (lane8 >> i & 1) + lax.rem(lax.div(me, 1 << i), 2)
    pop = pop & 3
    fr = jnp.where(pop == 0, 1.0, jnp.where(pop == 2, -1.0, 0.0))
    fi = jnp.where(pop == 1, -1.0, jnp.where(pop == 3, 1.0, 0.0))
    quarter = [(fr, fi), (fi, -fr), (-fr, -fi), (-fi, fr)]

    def power(block):
        picks = [quarter[(v.bit_count() + block.bit_count()) % 4] for v in range(n // 8)]
        return [jnp.concatenate([p[i] for p in picks], 0) if len(picks) > 1 else picks[0][i] for i in range(2)]

    fetched[1].wait()
    for g in range(4):
        st[plane(g), :] = level[g]
    fetched[2].wait()
    fetched[3].wait()
    planes = [[], []]
    for g in range(4):
        c, s = cos_sin(diag[0:1, :] * level[g])
        re, im = wave[0, g], wave[1, g]
        re, im = re * c + im * s, im * c - re * s
        pr, pi = power(g)
        planes[0].append(re * pr - im * pi)
        planes[1].append(im * pr + re * pi)

    def mix_blocks(xs, turn):
        xs[0], xs[2] = mix_pair(xs[0], xs[2], turn)
        xs[1], xs[3] = mix_pair(xs[1], xs[3], turn)
        xs[0], xs[1] = mix_pair(xs[0], xs[1], turn)
        xs[2], xs[3] = mix_pair(xs[2], xs[3], turn)
        return xs

    def columns(x):
        return [x[:, i : i + n] for i in range(0, x.shape[1], n)]

    for p in range(2):
        x = times_right(jnp.concatenate(planes[p], 0), tables[0])
        x = jnp.concatenate([x[g * n : (g + 1) * n] for g in range(4)], 1)
        x = times_left(tables[1], x)
        for g, x in enumerate(mix_blocks(columns(x), angle[0][OUTER])):
            s1[plane(p * 4 + g), :] = x
    pl.semaphore_wait(barrier, n - 1)
    send(st, rt, 0, LOW)
    send(s1, r1, 1, FULL)

    for g in range(4):
        st[plane(4 + g), :] = level[g].T
    send(st, rt, 2, HIGH)

    tables[2] = left_weights(turn_table(n, device_turns(0)))
    tables[3] = left_weights(turn_table(n, device_turns(1)))
    tables[4] = left_weights(turn_table(n, lane_turns(1)))

    arrive(rt, 0, LOW)
    for g in range(4):
        c, s = cos_sin(diag[1:2, :] * rt[plane(g), :])
        cs[0, g] = c
        cs[1, g] = s

    arrive(r1, 1, FULL)
    for p in range(2):
        x = jnp.concatenate([r1[plane(p * 4 + g), :] for g in range(4)], 1)
        x = times_left(tables[2], x)
        for g, x in enumerate(columns(x)):
            half[p, g] = x
    turned = [[], []]
    for g in range(4):
        re, im = half[0, g], half[1, g]
        c, s = cs[0, g], cs[1, g]
        turned[0].append(re * c + im * s)
        turned[1].append(im * c - re * s)
    for p in range(2):
        x = times_left(tables[3], jnp.concatenate(turned[p], 1))
        x = times_left_turned(tables[4], jnp.concatenate(columns(x), 0))
        for g, x in enumerate(mix_blocks(columns(x), angle[1][OUTER])):
            s2[plane((g % 2) * 4 + p * 2 + g // 2), :] = x
    send(s2, r2, 3, LOW)
    send(s2, r2, 4, HIGH)

    tables[5] = left_weights(turn_table(n, row_turns(1)))
    tables[6] = left_weights(turn_table(n, row_turns(2)))
    tables[7] = left_weights(turn_table(n, device_turns(2)))
    tables[8] = left_weights(turn_table(n, lane_turns(2)))

    lane1 = lax.broadcasted_iota(jnp.int32, (1, n), 1)
    own = jnp.sum(jnp.where(lane1 == me, diag[2:3, :], 0.0), axis=1, keepdims=True)
    arrive(rt, 2, HIGH)
    for g in range(4):
        c, s = cos_sin(own * rt[plane(4 + g), :].T)
        cs[0, g] = c
        cs[1, g] = s

    for q, part in enumerate((LOW, HIGH)):
        arrive(r2, 3 + q, part)
        pair = []
        for p in range(2):
            x = jnp.concatenate([r2[plane(q * 4 + p * 2 + g), :] for g in range(2)], 1)
            pair.append(columns(times_left(tables[5], x)))
        turned = [[], []]
        for g in range(2):
            re, im = pair[0][g], pair[1][g]
            c, s = cs[0, g * 2 + q], cs[1, g * 2 + q]
            turned[0].append(re * c + im * s)
            turned[1].append(im * c - re * s)
        for p in range(2):
            x = times_left(tables[6], jnp.concatenate(turned[p], 1))
            x = times_left_turned(tables[7], jnp.concatenate(columns(x), 0))
            for g, x in enumerate(mix_pair(*columns(x), angle[2][OUTER])):
                s3[plane(q * 4 + p * 2 + g), :] = x
        send(s3, r3, 5 + q, part)

    for q, part in enumerate((LOW, HIGH)):
        arrive(r3, 5 + q, part)
        for p in range(2):
            x = jnp.concatenate([r3[plane(q * 4 + p * 2 + g), :] for g in range(2)], 1)
            for g, x in enumerate(columns(times_left(tables[8], x))):
                half[p, g * 2 + q] = x.T
    for h in range(2):
        pairs = [mix_pair(half[p, h * 2], half[p, h * 2 + 1], angle[2][OUTER]) for p in range(2)]
        for q in range(2):
            re, im = pairs[0][q], pairs[1][q]
            pr, pi = power(h * 2 + q)
            out[0, h * 2 + q] = re * pr + im * pi
            out[1, h * 2 + q] = im * pr - re * pi

    sent(st, 0, LOW)
    sent(s1, 1, FULL)
    sent(st, 2, HIGH)
    for q, part in enumerate((LOW, HIGH)):
        sent(s2, 3 + q, part)
        sent(s3, 5 + q, part)


def fused(wave_parts, level_table, diagonal_angles, turn_angles, na, nb):
    n = na * nb
    f32 = jnp.float32
    V = pltpu.VMEM
    tiles = V((n * 8, n), f32)
    inputs = [
        pltpu.with_memory_space_constraint(x, pltpu.HBM)
        for x in (wave_parts, level_table, diagonal_angles, turn_angles)
    ]
    return pl.pallas_call(
        functools.partial(kernel, na, nb),
        out_shape=jax.ShapeDtypeStruct(wave_parts.shape, f32),
        in_specs=[pl.BlockSpec(memory_space=pltpu.HBM)] * 4,
        out_specs=pl.BlockSpec(memory_space=pltpu.VMEM),
        scratch_shapes=[
            V(wave_parts.shape, f32), V(level_table.shape, f32), V(diagonal_angles.shape, f32),
            pltpu.SMEM(turn_angles.shape, f32), pltpu.SemaphoreType.DMA((4,)),
            tiles, tiles, tiles, tiles, tiles, tiles, tiles, tiles,
            V((2,) + level_table.shape, f32), V(wave_parts.shape, f32),
            V((9, 2 * n, 2 * n), jnp.bfloat16),
            pltpu.SemaphoreType.DMA((7,)), pltpu.SemaphoreType.DMA((7,)),
        ],
        compiler_params=pltpu.CompilerParams(
            collective_id=0, has_side_effects=True, vmem_limit_bytes=32 * 1024 * 1024),
    )(*inputs)


def solution(mesh):
    na, nb = mesh.shape["qa"], mesh.shape["qb"]

    def each(wave_parts, level_table, diagonal_angles, turn_angles):
        return fused(wave_parts, level_table, diagonal_angles, turn_angles, na, nb)

    placed = (
        P("trial", ("qa", "qb"), None, None),
        P(("trial", "qa", "qb"), None, None),
        P("trial", None),
        P("trial", None),
    )
    return jax.shard_map(
        each,
        mesh=mesh,
        in_specs=placed,
        out_specs=P("trial", ("qa", "qb"), None, None),
        check_vma=False,
    )
```

```python
import functools

import jax
import jax.numpy as jnp
from jax import lax
from jax.experimental import pallas as pl
from jax.experimental.pallas import tpu as pltpu
from jax.sharding import PartitionSpec as P

LAYERS = 3
LANE, ROW, OUTER, MIDDLE = range(4)


def log2(count):
    return count.bit_length() - 1


def cos_sin(turn):
    half = 0.5 * turn
    y = half * half
    sine = -1 / 39916800
    for term in (1 / 362880, -1 / 5040, 1 / 120, -1 / 6, 1.0):
        sine = sine * y + term
    sine = sine * half
    cosine = 1 / 479001600
    for term in (-1 / 3628800, 1 / 40320, -1 / 720, 1 / 24, -0.5, 1.0):
        cosine = cosine * y + term
    return 1.0 - 2.0 * sine * sine, 2.0 * sine * cosine


def split(x):
    high = x.astype(jnp.bfloat16)
    return high, (x - high.astype(jnp.float32)).astype(jnp.bfloat16)


def dot(a, b, dims):
    return lax.dot_general(a, b, (dims, ((), ())), preferred_element_type=jnp.float32)


def right_weights(table):
    high, low = split(table)
    return jnp.concatenate(
        [jnp.concatenate([high, low], 1), jnp.concatenate([high, jnp.zeros_like(low)], 1)], 0)


def left_weights(table):
    high, low = split(table)
    return jnp.concatenate(
        [jnp.concatenate([high, high], 1), jnp.concatenate([low, jnp.zeros_like(low)], 1)], 0)


def times_right(x, weights):
    both = dot(jnp.concatenate(split(x), 1), weights, ((1,), (0,)))
    size = both.shape[1] // 2
    return both[:, :size] + both[:, size:]


def times_left(weights, x):
    both = dot(weights, jnp.concatenate(split(x), 0), ((1,), (0,)))
    size = both.shape[0] // 2
    return both[:size] + both[size:]


def times_left_turned(weights, x):
    both = dot(weights, jnp.concatenate(split(x), 1), ((1,), (1,)))
    size = both.shape[0] // 2
    return both[:size] + both[size:]


def turn_table(size, turns):
    out = lax.broadcasted_iota(jnp.int32, (8, size), 0)
    into = lax.broadcasted_iota(jnp.int32, (8, size), 1)
    table = None
    for i in range(3):
        c, s = turns[i]
        o, t = out >> i & 1, into >> i & 1
        factor = jnp.where(o == t, c, jnp.where(o > t, -s, s))
        table = factor if table is None else table * factor
    for i in range(3, log2(size)):
        c, s = turns[i]
        t = (into >> i & 1) == 0
        table = jnp.concatenate([_times(table, jnp.where(t, c, s)), _times(table, jnp.where(t, -s, c))], 0)
    return table


def _times(table, factor):
    rows = [table[i : i + 8] * factor for i in range(0, table.shape[0], 8)]
    return rows[0] if len(rows) == 1 else jnp.concatenate(rows, 0)


def mix_pair(u, v, turn):
    c, s = turn
    return c * u + s * v, c * v - s * u


def kernel(na, nb, wave_hbm, level_hbm, diag_hbm, turns_hbm, out, wave, level, diag, turns, in_sem,
           st, rt, s1, r1, s2, r2, s3, r3, cs, half, tables, send_sem, recv_sem):
    n = na * nb
    f32 = jnp.float32
    a = lax.axis_index("qa")
    b = lax.axis_index("qb")
    me = a * nb + b

    places = [lax.rem(b + j, nb) for j in range(nb)]
    away = sorted(range(1, nb), key=lambda j: -min(j, nb - j))

    def each_peer(visit):
        def step(i, carry, shifts):
            pa = lax.rem(a + i, na)
            for j in shifts:
                visit(pa * nb + places[j], {"qa": pa, "qb": places[j]})
            return carry

        step(0, 0, away)
        lax.fori_loop(1, na, functools.partial(step, shifts=[0] + away), 0)

    def each_peer_by_plane(visit):
        def step(i, carry, planes):
            pa = lax.rem(a + i, na)
            for pb in planes:
                visit(pa * nb + pb, {"qa": pa, "qb": pb})
            return carry

        for j in away:
            visit(a * nb + places[j], {"qa": a, "qb": places[j]})
        for planes in (range(nb // 2), range(nb // 2, nb)):
            lax.fori_loop(1, na, functools.partial(step, planes=planes), 0)

    fetched = [
        pltpu.make_async_copy(src, dst, in_sem.at[i])
        for i, (src, dst) in enumerate(
            ((turns_hbm, turns), (level_hbm, level), (diag_hbm, diag), (wave_hbm, wave)))
    ]
    for copy in fetched:
        copy.start()

    barrier = pltpu.get_barrier_semaphore()

    def greet(peer, to):
        pl.semaphore_signal(barrier, inc=1, device_id=to, device_id_type=pl.DeviceIdType.MESH)

    each_peer(greet)

    def tile(ref, i, part):
        first, count = part
        step = ref.shape[0] // n
        return ref.at[pl.ds(pl.multiple_of(i * step, 8) + first, count)]

    def send(src, dst, which, part, each=each_peer):
        def visit(peer, to):
            pltpu.make_async_remote_copy(
                src_ref=tile(src, peer, part), dst_ref=tile(dst, me, part), send_sem=send_sem.at[which],
                recv_sem=recv_sem.at[which], device_id=to, device_id_type=pl.DeviceIdType.MESH).start()

        each(visit)
        step = src.shape[0] // n
        own = pl.ds(pl.multiple_of(me * step, 8), step)
        dst[own, :] = src[own, :]

    def total(ref, sem, part):
        whole = ref.at[pl.ds(0, (n - 1) * part[1])]
        return pltpu.make_async_copy(whole, whole, sem)

    def arrive(dst, which, part):
        total(dst, recv_sem.at[which], part).wait()

    def sent(src, which, part):
        total(src, send_sem.at[which], part).wait()

    WITH_LEVELS, LOW, HIGH = (0, 12), (0, 4), (4, 4)

    def plane(j, step=8):
        return pl.ds(j, n, stride=step)

    fetched[0].wait()
    angle = [[cos_sin(jnp.full((1, n), turns[layer, g], f32)) for g in range(4)] for layer in range(LAYERS)]
    bits = log2(n)

    def lane_turns(layer):
        return [angle[layer][LANE]] * bits

    def row_turns(layer):
        return [angle[layer][ROW]] * bits

    def device_turns(layer):
        return [angle[layer][MIDDLE]] * log2(nb) + [angle[layer][OUTER]] * log2(na)

    def back(turn_list):
        return [(c, -s) for c, s in turn_list]

    tables[0] = right_weights(turn_table(n, back(lane_turns(0))))
    tables[1] = left_weights(turn_table(n, row_turns(0)))

    pop = jnp.zeros((8, n), jnp.int32)
    row8 = lax.broadcasted_iota(jnp.int32, (8, n), 0)
    lane8 = lax.broadcasted_iota(jnp.int32, (8, n), 1)
    for i in range(3):
        pop = pop + (row8 >> i & 1)
    for i in range(bits):
        pop = pop + (lane8 >> i & 1) + lax.rem(lax.div(me, 1 << i), 2)
    pop = pop & 3
    fr = jnp.where(pop == 0, 1.0, jnp.where(pop == 2, -1.0, 0.0))
    fi = jnp.where(pop == 1, -1.0, jnp.where(pop == 3, 1.0, 0.0))
    quarter = [(fr, fi), (fi, -fr), (-fr, -fi), (-fi, fr)]

    def power(block):
        picks = [quarter[(v.bit_count() + block.bit_count()) % 4] for v in range(n // 8)]
        return [jnp.concatenate([p[i] for p in picks], 0) if len(picks) > 1 else picks[0][i] for i in range(2)]

    fetched[1].wait()
    for g in range(4):
        s1[plane(8 + g, 16), :] = level[g]
        st[plane(g), :] = level[g].T
    fetched[2].wait()
    fetched[3].wait()
    planes = [[], []]
    for g in range(4):
        c, s = cos_sin(diag[0:1, :] * level[g])
        re, im = wave[0, g], wave[1, g]
        re, im = re * c + im * s, im * c - re * s
        pr, pi = power(g)
        planes[0].append(re * pr - im * pi)
        planes[1].append(im * pr + re * pi)

    def mix_blocks(xs, turn):
        xs[0], xs[2] = mix_pair(xs[0], xs[2], turn)
        xs[1], xs[3] = mix_pair(xs[1], xs[3], turn)
        xs[0], xs[1] = mix_pair(xs[0], xs[1], turn)
        xs[2], xs[3] = mix_pair(xs[2], xs[3], turn)
        return xs

    def columns(x):
        return [x[:, i : i + n] for i in range(0, x.shape[1], n)]

    for p in range(2):
        x = times_right(jnp.concatenate(planes[p], 0), tables[0])
        x = jnp.concatenate([x[g * n : (g + 1) * n] for g in range(4)], 1)
        x = times_left(tables[1], x)
        for g, x in enumerate(mix_blocks(columns(x), angle[0][OUTER])):
            s1[plane(p * 4 + g, 16), :] = x
    pl.semaphore_wait(barrier, n - 1)
    send(s1, r1, 0, WITH_LEVELS)
    send(st, rt, 1, LOW)

    tables[2] = left_weights(turn_table(n, device_turns(0)))
    tables[3] = left_weights(turn_table(n, device_turns(1)))
    tables[4] = left_weights(turn_table(n, lane_turns(1)))

    arrive(r1, 0, WITH_LEVELS)
    for p in range(2):
        x = jnp.concatenate([r1[plane(p * 4 + g, 16), :] for g in range(4)], 1)
        x = times_left(tables[2], x)
        for g, x in enumerate(columns(x)):
            half[p, g] = x
    turned = [[], []]
    for g in range(4):
        re, im = half[0, g], half[1, g]
        c, s = cos_sin(diag[1:2, :] * r1[plane(8 + g, 16), :])
        turned[0].append(re * c + im * s)
        turned[1].append(im * c - re * s)
    for p in range(2):
        x = times_left(tables[3], jnp.concatenate(turned[p], 1))
        x = times_left_turned(tables[4], jnp.concatenate(columns(x), 0))
        for g, x in enumerate(mix_blocks(columns(x), angle[1][OUTER])):
            s2[plane((g % 2) * 4 + p * 2 + g // 2), :] = x
    send(s2, r2, 2, LOW)
    send(s2, r2, 3, HIGH)

    tables[5] = left_weights(turn_table(n, row_turns(1)))
    tables[6] = left_weights(turn_table(n, row_turns(2)))
    tables[7] = left_weights(turn_table(n, device_turns(2)))
    tables[8] = left_weights(turn_table(n, lane_turns(2)))

    lane1 = lax.broadcasted_iota(jnp.int32, (1, n), 1)
    own = jnp.sum(jnp.where(lane1 == me, diag[2:3, :], 0.0), axis=1, keepdims=True)
    arrive(rt, 1, LOW)
    for g in range(4):
        c, s = cos_sin(own * rt[plane(g), :].T)
        cs[0, g] = c
        cs[1, g] = s

    for q, part in enumerate((LOW, HIGH)):
        arrive(r2, 2 + q, part)
        pair = []
        for p in range(2):
            x = jnp.concatenate([r2[plane(q * 4 + p * 2 + g), :] for g in range(2)], 1)
            pair.append(columns(times_left(tables[5], x)))
        turned = [[], []]
        for g in range(2):
            re, im = pair[0][g], pair[1][g]
            c, s = cs[0, g * 2 + q], cs[1, g * 2 + q]
            turned[0].append(re * c + im * s)
            turned[1].append(im * c - re * s)
        for p in range(2):
            x = times_left(tables[6], jnp.concatenate(turned[p], 1))
            x = times_left_turned(tables[7], jnp.concatenate(columns(x), 0))
            for g, x in enumerate(mix_pair(*columns(x), angle[2][OUTER])):
                s3[plane(q * 4 + p * 2 + g), :] = x
        send(s3, r3, 4 + q, part, (each_peer, each_peer_by_plane)[q])

    for q, part in enumerate((LOW, HIGH)):
        arrive(r3, 4 + q, part)
        for p in range(2):
            x = jnp.concatenate([r3[plane(q * 4 + p * 2 + g), :] for g in range(2)], 1)
            for g, x in enumerate(columns(times_left(tables[8], x))):
                half[p, g * 2 + q] = x.T
    for h in range(2):
        pairs = [mix_pair(half[p, h * 2], half[p, h * 2 + 1], angle[2][OUTER]) for p in range(2)]
        for q in range(2):
            re, im = pairs[0][q], pairs[1][q]
            pr, pi = power(h * 2 + q)
            out[0, h * 2 + q] = re * pr + im * pi
            out[1, h * 2 + q] = im * pr - re * pi

    sent(s1, 0, WITH_LEVELS)
    sent(st, 1, LOW)
    for q, part in enumerate((LOW, HIGH)):
        sent(s2, 2 + q, part)
        sent(s3, 4 + q, part)


def fused(wave_parts, level_table, diagonal_angles, turn_angles, na, nb):
    n = na * nb
    f32 = jnp.float32
    V = pltpu.VMEM
    tiles, tall = V((n * 8, n), f32), V((n * 16, n), f32)
    inputs = [
        pltpu.with_memory_space_constraint(x, pltpu.HBM)
        for x in (wave_parts, level_table, diagonal_angles, turn_angles)
    ]
    return pl.pallas_call(
        functools.partial(kernel, na, nb),
        out_shape=jax.ShapeDtypeStruct(wave_parts.shape, f32),
        in_specs=[pl.BlockSpec(memory_space=pltpu.HBM)] * 4,
        out_specs=pl.BlockSpec(memory_space=pltpu.VMEM),
        scratch_shapes=[
            V(wave_parts.shape, f32), V(level_table.shape, f32), V(diagonal_angles.shape, f32),
            pltpu.SMEM(turn_angles.shape, f32), pltpu.SemaphoreType.DMA((4,)),
            tiles, tiles, tall, tall, tiles, tiles, tiles, tiles,
            V((2,) + level_table.shape, f32), V(wave_parts.shape, f32),
            V((9, 2 * n, 2 * n), jnp.bfloat16),
            pltpu.SemaphoreType.DMA((6,)), pltpu.SemaphoreType.DMA((6,)),
        ],
        compiler_params=pltpu.CompilerParams(
            collective_id=0, has_side_effects=True, vmem_limit_bytes=32 * 1024 * 1024),
    )(*inputs)


def solution(mesh):
    na, nb = mesh.shape["qa"], mesh.shape["qb"]

    def each(wave_parts, level_table, diagonal_angles, turn_angles):
        return fused(wave_parts, level_table, diagonal_angles, turn_angles, na, nb)

    placed = (
        P("trial", ("qa", "qb"), None, None),
        P(("trial", "qa", "qb"), None, None),
        P("trial", None),
        P("trial", None),
    )
    return jax.shard_map(
        each,
        mesh=mesh,
        in_specs=placed,
        out_specs=P("trial", ("qa", "qb"), None, None),
        check_vma=False,
    )
```

```python
import functools

import jax
import jax.numpy as jnp
from jax import lax
from jax.experimental import pallas as pl
from jax.experimental.pallas import tpu as pltpu
from jax.sharding import PartitionSpec as P

LAYERS = 3
LANE, ROW, OUTER, MIDDLE = range(4)


def log2(count):
    return count.bit_length() - 1


def cos_sin(turn):
    half = 0.5 * turn
    y = half * half
    sine = -1 / 39916800
    for term in (1 / 362880, -1 / 5040, 1 / 120, -1 / 6, 1.0):
        sine = sine * y + term
    sine = sine * half
    cosine = 1 / 479001600
    for term in (-1 / 3628800, 1 / 40320, -1 / 720, 1 / 24, -0.5, 1.0):
        cosine = cosine * y + term
    return 1.0 - 2.0 * sine * sine, 2.0 * sine * cosine


def split(x):
    high = x.astype(jnp.bfloat16)
    return high, (x - high.astype(jnp.float32)).astype(jnp.bfloat16)


def dot(a, b, dims):
    return lax.dot_general(a, b, (dims, ((), ())), preferred_element_type=jnp.float32)


def right_weights(table):
    high, low = split(table)
    return jnp.concatenate(
        [jnp.concatenate([high, low], 1), jnp.concatenate([high, jnp.zeros_like(low)], 1)], 0)


def left_weights(table):
    high, low = split(table)
    return jnp.concatenate(
        [jnp.concatenate([high, high], 1), jnp.concatenate([low, jnp.zeros_like(low)], 1)], 0)


def times_right(x, weights):
    both = dot(jnp.concatenate(split(x), 1), weights, ((1,), (0,)))
    size = both.shape[1] // 2
    return both[:, :size] + both[:, size:]


def times_left(weights, x):
    both = dot(weights, jnp.concatenate(split(x), 0), ((1,), (0,)))
    size = both.shape[0] // 2
    return both[:size] + both[size:]


def times_left_turned(weights, x):
    both = dot(weights, jnp.concatenate(split(x), 1), ((1,), (1,)))
    size = both.shape[0] // 2
    return both[:size] + both[size:]


def turn_table(size, turns):
    out = lax.broadcasted_iota(jnp.int32, (8, size), 0)
    into = lax.broadcasted_iota(jnp.int32, (8, size), 1)
    table = None
    for i in range(3):
        c, s = turns[i]
        o, t = out >> i & 1, into >> i & 1
        factor = jnp.where(o == t, c, jnp.where(o > t, -s, s))
        table = factor if table is None else table * factor
    for i in range(3, log2(size)):
        c, s = turns[i]
        t = (into >> i & 1) == 0
        table = jnp.concatenate([_times(table, jnp.where(t, c, s)), _times(table, jnp.where(t, -s, c))], 0)
    return table


def _times(table, factor):
    rows = [table[i : i + 8] * factor for i in range(0, table.shape[0], 8)]
    return rows[0] if len(rows) == 1 else jnp.concatenate(rows, 0)


def mix_pair(u, v, turn):
    c, s = turn
    return c * u + s * v, c * v - s * u


def kernel(na, nb, wave_hbm, level_hbm, diag_hbm, turns_hbm, out, wave, level, diag, turns, in_sem,
           st, rt, s1, r1, s2, r2, s3, r3, cs, half, tables, send_sem, recv_sem):
    n = na * nb
    f32 = jnp.float32
    a = lax.axis_index("qa")
    b = lax.axis_index("qb")
    trial = lax.axis_index("trial")
    me = a * nb + b

    places = [lax.rem(b + j, nb) for j in range(nb)]
    away = sorted(range(1, nb), key=lambda j: -min(j, nb - j))

    def each_peer(visit, farthest=False):
        def step(i, carry, shifts):
            pa = lax.rem(a + i, na)
            for j in shifts:
                visit(pa * nb + places[j], {"qa": pa, "qb": places[j]})
            return carry

        row = functools.partial(step, shifts=[0] + away)
        if farthest:
            lax.fori_loop(na // 2, na, row, 0)
        step(0, 0, away)
        lax.fori_loop(1, na // 2 if farthest else na, row, 0)

    def each_peer_by_plane(visit):
        start = trial * (nb // 2)
        quarter = max(1, nb // 4)

        def step(i, carry, planes):
            pa = lax.rem(a + i, na)
            for j in planes:
                pb = lax.rem(start + j, nb)
                visit(pa * nb + pb, {"qa": pa, "qb": pb})
            return carry

        for j in away:
            visit(a * nb + places[j], {"qa": a, "qb": places[j]})
        for planes in (range(quarter), range(quarter, nb // 2), range(nb // 2, nb)):
            lax.fori_loop(1, na, functools.partial(step, planes=planes), 0)

    fetched = [
        pltpu.make_async_copy(src, dst, in_sem.at[i])
        for i, (src, dst) in enumerate(
            ((turns_hbm, turns), (level_hbm, level), (diag_hbm, diag), (wave_hbm, wave)))
    ]
    for copy in fetched:
        copy.start()

    barrier = pltpu.get_barrier_semaphore()

    def greet(peer, to):
        pl.semaphore_signal(barrier, inc=1, device_id=to, device_id_type=pl.DeviceIdType.MESH)

    each_peer(greet, farthest=True)

    def tile(ref, i, part):
        first, count = part
        step = ref.shape[0] // n
        return ref.at[pl.ds(pl.multiple_of(i * step, 8) + first, count)]

    def send(src, dst, which, part, each=each_peer):
        def visit(peer, to):
            pltpu.make_async_remote_copy(
                src_ref=tile(src, peer, part), dst_ref=tile(dst, me, part), send_sem=send_sem.at[which],
                recv_sem=recv_sem.at[which], device_id=to, device_id_type=pl.DeviceIdType.MESH).start()

        each(visit)
        step = src.shape[0] // n
        own = pl.ds(pl.multiple_of(me * step, 8), step)
        dst[own, :] = src[own, :]

    def total(ref, sem, part):
        whole = ref.at[pl.ds(0, (n - 1) * part[1])]
        return pltpu.make_async_copy(whole, whole, sem)

    def arrive(dst, which, part):
        total(dst, recv_sem.at[which], part).wait()

    def sent(src, which, part):
        total(src, send_sem.at[which], part).wait()

    WITH_LEVELS, LOW, HIGH = (0, 12), (0, 4), (4, 4)

    def plane(j, step=8):
        return pl.ds(j, n, stride=step)

    fetched[0].wait()
    angle = [[cos_sin(jnp.full((1, n), turns[layer, g], f32)) for g in range(4)] for layer in range(LAYERS)]
    bits = log2(n)

    def lane_turns(layer):
        return [angle[layer][LANE]] * bits

    def row_turns(layer):
        return [angle[layer][ROW]] * bits

    def device_turns(layer):
        return [angle[layer][MIDDLE]] * log2(nb) + [angle[layer][OUTER]] * log2(na)

    def back(turn_list):
        return [(c, -s) for c, s in turn_list]

    tables[0] = right_weights(turn_table(n, back(lane_turns(0))))
    tables[1] = left_weights(turn_table(n, row_turns(0)))

    pop = jnp.zeros((8, n), jnp.int32)
    row8 = lax.broadcasted_iota(jnp.int32, (8, n), 0)
    lane8 = lax.broadcasted_iota(jnp.int32, (8, n), 1)
    for i in range(3):
        pop = pop + (row8 >> i & 1)
    for i in range(bits):
        pop = pop + (lane8 >> i & 1) + lax.rem(lax.div(me, 1 << i), 2)
    pop = pop & 3
    fr = jnp.where(pop == 0, 1.0, jnp.where(pop == 2, -1.0, 0.0))
    fi = jnp.where(pop == 1, -1.0, jnp.where(pop == 3, 1.0, 0.0))
    quarter = [(fr, fi), (fi, -fr), (-fr, -fi), (-fi, fr)]

    def power(block):
        picks = [quarter[(v.bit_count() + block.bit_count()) % 4] for v in range(n // 8)]
        return [jnp.concatenate([p[i] for p in picks], 0) if len(picks) > 1 else picks[0][i] for i in range(2)]

    fetched[1].wait()
    for g in range(4):
        s1[plane(8 + g, 16), :] = level[g]
        st[plane(g), :] = level[g].T
    fetched[2].wait()
    fetched[3].wait()
    planes = [[], []]
    for g in range(4):
        c, s = cos_sin(diag[0:1, :] * level[g])
        re, im = wave[0, g], wave[1, g]
        re, im = re * c + im * s, im * c - re * s
        pr, pi = power(g)
        planes[0].append(re * pr - im * pi)
        planes[1].append(im * pr + re * pi)

    def mix_blocks(xs, turn):
        xs[0], xs[2] = mix_pair(xs[0], xs[2], turn)
        xs[1], xs[3] = mix_pair(xs[1], xs[3], turn)
        xs[0], xs[1] = mix_pair(xs[0], xs[1], turn)
        xs[2], xs[3] = mix_pair(xs[2], xs[3], turn)
        return xs

    def columns(x):
        return [x[:, i : i + n] for i in range(0, x.shape[1], n)]

    for p in range(2):
        x = times_right(jnp.concatenate(planes[p], 0), tables[0])
        x = jnp.concatenate([x[g * n : (g + 1) * n] for g in range(4)], 1)
        x = times_left(tables[1], x)
        for g, x in enumerate(mix_blocks(columns(x), angle[0][OUTER])):
            s1[plane(p * 4 + g, 16), :] = x
    pl.semaphore_wait(barrier, n - 1)
    send(s1, r1, 0, WITH_LEVELS)
    send(st, rt, 1, LOW)

    tables[2] = left_weights(turn_table(n, device_turns(0)))
    tables[3] = left_weights(turn_table(n, device_turns(1)))
    tables[4] = left_weights(turn_table(n, lane_turns(1)))

    arrive(r1, 0, WITH_LEVELS)
    for p in range(2):
        x = jnp.concatenate([r1[plane(p * 4 + g, 16), :] for g in range(4)], 1)
        x = times_left(tables[2], x)
        for g, x in enumerate(columns(x)):
            half[p, g] = x
    turned = [[], []]
    for g in range(4):
        re, im = half[0, g], half[1, g]
        c, s = cos_sin(diag[1:2, :] * r1[plane(8 + g, 16), :])
        turned[0].append(re * c + im * s)
        turned[1].append(im * c - re * s)
    for p in range(2):
        x = times_left(tables[3], jnp.concatenate(turned[p], 1))
        x = times_left_turned(tables[4], jnp.concatenate(columns(x), 0))
        for g, x in enumerate(mix_blocks(columns(x), angle[1][OUTER])):
            s2[plane((g % 2) * 4 + p * 2 + g // 2), :] = x
    send(s2, r2, 2, LOW)
    send(s2, r2, 3, HIGH)

    tables[5] = left_weights(turn_table(n, row_turns(1)))
    tables[6] = left_weights(turn_table(n, row_turns(2)))
    tables[7] = left_weights(turn_table(n, device_turns(2)))
    tables[8] = left_weights(turn_table(n, lane_turns(2)))

    lane1 = lax.broadcasted_iota(jnp.int32, (1, n), 1)
    own = jnp.sum(jnp.where(lane1 == me, diag[2:3, :], 0.0), axis=1, keepdims=True)
    arrive(rt, 1, LOW)
    for g in range(4):
        c, s = cos_sin(own * rt[plane(g), :].T)
        cs[0, g] = c
        cs[1, g] = s

    for q, part in enumerate((LOW, HIGH)):
        arrive(r2, 2 + q, part)
        pair = []
        for p in range(2):
            x = jnp.concatenate([r2[plane(q * 4 + p * 2 + g), :] for g in range(2)], 1)
            pair.append(columns(times_left(tables[5], x)))
        turned = [[], []]
        for g in range(2):
            re, im = pair[0][g], pair[1][g]
            c, s = cs[0, g * 2 + q], cs[1, g * 2 + q]
            turned[0].append(re * c + im * s)
            turned[1].append(im * c - re * s)
        for p in range(2):
            x = times_left(tables[6], jnp.concatenate(turned[p], 1))
            x = times_left_turned(tables[7], jnp.concatenate(columns(x), 0))
            for g, x in enumerate(mix_pair(*columns(x), angle[2][OUTER])):
                s3[plane(q * 4 + p * 2 + g), :] = x
        send(s3, r3, 4 + q, part, (each_peer, each_peer_by_plane)[q])

    for q, part in enumerate((LOW, HIGH)):
        arrive(r3, 4 + q, part)
        for p in range(2):
            x = jnp.concatenate([r3[plane(q * 4 + p * 2 + g), :] for g in range(2)], 1)
            for g, x in enumerate(columns(times_left(tables[8], x))):
                half[p, g * 2 + q] = x.T
    for h in range(2):
        pairs = [mix_pair(half[p, h * 2], half[p, h * 2 + 1], angle[2][OUTER]) for p in range(2)]
        for q in range(2):
            re, im = pairs[0][q], pairs[1][q]
            pr, pi = power(h * 2 + q)
            out[0, h * 2 + q] = re * pr + im * pi
            out[1, h * 2 + q] = im * pr - re * pi

    sent(s1, 0, WITH_LEVELS)
    sent(st, 1, LOW)
    for q, part in enumerate((LOW, HIGH)):
        sent(s2, 2 + q, part)
        sent(s3, 4 + q, part)


def fused(wave_parts, level_table, diagonal_angles, turn_angles, na, nb):
    n = na * nb
    f32 = jnp.float32
    V = pltpu.VMEM
    tiles, tall = V((n * 8, n), f32), V((n * 16, n), f32)
    inputs = [
        pltpu.with_memory_space_constraint(x, pltpu.HBM)
        for x in (wave_parts, level_table, diagonal_angles, turn_angles)
    ]
    return pl.pallas_call(
        functools.partial(kernel, na, nb),
        out_shape=jax.ShapeDtypeStruct(wave_parts.shape, f32),
        in_specs=[pl.BlockSpec(memory_space=pltpu.HBM)] * 4,
        out_specs=pl.BlockSpec(memory_space=pltpu.VMEM),
        scratch_shapes=[
            V(wave_parts.shape, f32), V(level_table.shape, f32), V(diagonal_angles.shape, f32),
            pltpu.SMEM(turn_angles.shape, f32), pltpu.SemaphoreType.DMA((4,)),
            tiles, tiles, tall, tall, tiles, tiles, tiles, tiles,
            V((2,) + level_table.shape, f32), V(wave_parts.shape, f32),
            V((9, 2 * n, 2 * n), jnp.bfloat16),
            pltpu.SemaphoreType.DMA((6,)), pltpu.SemaphoreType.DMA((6,)),
        ],
        compiler_params=pltpu.CompilerParams(
            collective_id=0, has_side_effects=True, vmem_limit_bytes=32 * 1024 * 1024),
    )(*inputs)


def solution(mesh):
    na, nb = mesh.shape["qa"], mesh.shape["qb"]

    def each(wave_parts, level_table, diagonal_angles, turn_angles):
        return fused(wave_parts, level_table, diagonal_angles, turn_angles, na, nb)

    placed = (
        P("trial", ("qa", "qb"), None, None),
        P(("trial", "qa", "qb"), None, None),
        P("trial", None),
        P("trial", None),
    )
    return jax.shard_map(
        each,
        mesh=mesh,
        in_specs=placed,
        out_specs=P("trial", ("qa", "qb"), None, None),
        check_vma=False,
    )
```

```python
import functools

import jax
import jax.numpy as jnp
from jax import lax
from jax.experimental import pallas as pl
from jax.experimental.pallas import tpu as pltpu
from jax.sharding import PartitionSpec as P

LAYERS = 3
LANE, ROW, OUTER, MIDDLE = range(4)


def log2(count):
    return count.bit_length() - 1


def cos_sin(turn):
    half = 0.5 * turn
    y = half * half
    sine = -1 / 39916800
    for term in (1 / 362880, -1 / 5040, 1 / 120, -1 / 6, 1.0):
        sine = sine * y + term
    sine = sine * half
    cosine = 1 / 479001600
    for term in (-1 / 3628800, 1 / 40320, -1 / 720, 1 / 24, -0.5, 1.0):
        cosine = cosine * y + term
    return 1.0 - 2.0 * sine * sine, 2.0 * sine * cosine


def split(x):
    high = x.astype(jnp.bfloat16)
    return high, (x - high.astype(jnp.float32)).astype(jnp.bfloat16)


def dot(a, b, dims):
    return lax.dot_general(a, b, (dims, ((), ())), preferred_element_type=jnp.float32)


def right_weights(table):
    high, low = split(table)
    return jnp.concatenate(
        [jnp.concatenate([high, low], 1), jnp.concatenate([high, jnp.zeros_like(low)], 1)], 0)


def left_weights(table):
    high, low = split(table)
    return jnp.concatenate(
        [jnp.concatenate([high, high], 1), jnp.concatenate([low, jnp.zeros_like(low)], 1)], 0)


def times_right(x, weights):
    both = dot(jnp.concatenate(split(x), 1), weights, ((1,), (0,)))
    size = both.shape[1] // 2
    return both[:, :size] + both[:, size:]


def times_left(weights, x):
    both = dot(weights, jnp.concatenate(split(x), 0), ((1,), (0,)))
    size = both.shape[0] // 2
    return both[:size] + both[size:]


def times_left_turned(weights, x):
    both = dot(weights, jnp.concatenate(split(x), 1), ((1,), (1,)))
    size = both.shape[0] // 2
    return both[:size] + both[size:]


def turn_table(size, turns):
    out = lax.broadcasted_iota(jnp.int32, (8, size), 0)
    into = lax.broadcasted_iota(jnp.int32, (8, size), 1)
    table = None
    for i in range(3):
        c, s = turns[i]
        o, t = out >> i & 1, into >> i & 1
        factor = jnp.where(o == t, c, jnp.where(o > t, -s, s))
        table = factor if table is None else table * factor
    for i in range(3, log2(size)):
        c, s = turns[i]
        t = (into >> i & 1) == 0
        table = jnp.concatenate([_times(table, jnp.where(t, c, s)), _times(table, jnp.where(t, -s, c))], 0)
    return table


def _times(table, factor):
    rows = [table[i : i + 8] * factor for i in range(0, table.shape[0], 8)]
    return rows[0] if len(rows) == 1 else jnp.concatenate(rows, 0)


def mix_pair(u, v, turn):
    c, s = turn
    return c * u + s * v, c * v - s * u


def kernel(na, nb, wave_hbm, level_hbm, diag_hbm, turns_hbm, out, wave, level, diag, turns, in_sem,
           st, rt, s1, r1, s2, r2, s3, r3, cs, half, tables, send_sem, recv_sem):
    n = na * nb
    f32 = jnp.float32
    a = lax.axis_index("qa")
    b = lax.axis_index("qb")
    me = a * nb + b

    places = [lax.rem(b + j, nb) for j in range(nb)]
    away = sorted(range(1, nb), key=lambda j: -min(j, nb - j))

    def each_peer(visit):
        def step(i, carry, shifts):
            pa = lax.rem(a + i, na)
            for j in shifts:
                visit(pa * nb + places[j], {"qa": pa, "qb": places[j]})
            return carry

        step(0, 0, away)
        lax.fori_loop(1, na, functools.partial(step, shifts=[0] + away), 0)

    def each_peer_by_plane(visit):
        trial = lax.axis_index("trial")
        order = [(1 - trial) * j + trial * places[shift] for j, shift in enumerate(away + [0])]

        def step(i, carry, planes):
            pa = lax.rem(a + i, na)
            for pb in planes:
                visit(pa * nb + pb, {"qa": pa, "qb": pb})
            return carry

        for j in away:
            visit(a * nb + places[j], {"qa": a, "qb": places[j]})
        for planes in (order[: nb // 2], order[nb // 2 :]):
            lax.fori_loop(1, na, functools.partial(step, planes=planes), 0)

    fetched = [
        pltpu.make_async_copy(src, dst, in_sem.at[i])
        for i, (src, dst) in enumerate(
            ((turns_hbm, turns), (level_hbm, level), (diag_hbm, diag), (wave_hbm, wave)))
    ]
    for copy in fetched:
        copy.start()

    barrier = pltpu.get_barrier_semaphore()

    def greet(peer, to):
        pl.semaphore_signal(barrier, inc=1, device_id=to, device_id_type=pl.DeviceIdType.MESH)

    each_peer(greet)

    def tile(ref, i, part):
        first, count = part
        step = ref.shape[0] // n
        return ref.at[pl.ds(pl.multiple_of(i * step, 8) + first, count)]

    def send(src, dst, which, part, each=each_peer):
        def visit(peer, to):
            pltpu.make_async_remote_copy(
                src_ref=tile(src, peer, part), dst_ref=tile(dst, me, part), send_sem=send_sem.at[which],
                recv_sem=recv_sem.at[which], device_id=to, device_id_type=pl.DeviceIdType.MESH).start()

        each(visit)
        step = src.shape[0] // n
        own = pl.ds(pl.multiple_of(me * step, 8), step)
        dst[own, :] = src[own, :]

    def total(ref, sem, part):
        whole = ref.at[pl.ds(0, (n - 1) * part[1])]
        return pltpu.make_async_copy(whole, whole, sem)

    def arrive(dst, which, part):
        total(dst, recv_sem.at[which], part).wait()

    def sent(src, which, part):
        total(src, send_sem.at[which], part).wait()

    WITH_LEVELS, LOW, HIGH = (0, 12), (0, 4), (4, 4)

    def plane(j, step=8):
        return pl.ds(j, n, stride=step)

    fetched[0].wait()
    angle = [[cos_sin(jnp.full((1, n), turns[layer, g], f32)) for g in range(4)] for layer in range(LAYERS)]
    bits = log2(n)

    def lane_turns(layer):
        return [angle[layer][LANE]] * bits

    def row_turns(layer):
        return [angle[layer][ROW]] * bits

    def device_turns(layer):
        return [angle[layer][MIDDLE]] * log2(nb) + [angle[layer][OUTER]] * log2(na)

    def back(turn_list):
        return [(c, -s) for c, s in turn_list]

    tables[0] = right_weights(turn_table(n, back(lane_turns(0))))
    tables[1] = left_weights(turn_table(n, row_turns(0)))

    pop = jnp.zeros((8, n), jnp.int32)
    row8 = lax.broadcasted_iota(jnp.int32, (8, n), 0)
    lane8 = lax.broadcasted_iota(jnp.int32, (8, n), 1)
    for i in range(3):
        pop = pop + (row8 >> i & 1)
    for i in range(bits):
        pop = pop + (lane8 >> i & 1) + lax.rem(lax.div(me, 1 << i), 2)
    pop = pop & 3
    fr = jnp.where(pop == 0, 1.0, jnp.where(pop == 2, -1.0, 0.0))
    fi = jnp.where(pop == 1, -1.0, jnp.where(pop == 3, 1.0, 0.0))
    quarter = [(fr, fi), (fi, -fr), (-fr, -fi), (-fi, fr)]

    def power(block):
        picks = [quarter[(v.bit_count() + block.bit_count()) % 4] for v in range(n // 8)]
        return [jnp.concatenate([p[i] for p in picks], 0) if len(picks) > 1 else picks[0][i] for i in range(2)]

    fetched[1].wait()
    for g in range(4):
        s1[plane(8 + g, 16), :] = level[g]
        st[plane(g), :] = level[g].T
    fetched[2].wait()
    fetched[3].wait()
    planes = [[], []]
    for g in range(4):
        c, s = cos_sin(diag[0:1, :] * level[g])
        re, im = wave[0, g], wave[1, g]
        re, im = re * c + im * s, im * c - re * s
        pr, pi = power(g)
        planes[0].append(re * pr - im * pi)
        planes[1].append(im * pr + re * pi)

    def mix_blocks(xs, turn):
        xs[0], xs[2] = mix_pair(xs[0], xs[2], turn)
        xs[1], xs[3] = mix_pair(xs[1], xs[3], turn)
        xs[0], xs[1] = mix_pair(xs[0], xs[1], turn)
        xs[2], xs[3] = mix_pair(xs[2], xs[3], turn)
        return xs

    def columns(x):
        return [x[:, i : i + n] for i in range(0, x.shape[1], n)]

    for p in range(2):
        x = times_right(jnp.concatenate(planes[p], 0), tables[0])
        x = jnp.concatenate([x[g * n : (g + 1) * n] for g in range(4)], 1)
        x = times_left(tables[1], x)
        for g, x in enumerate(mix_blocks(columns(x), angle[0][OUTER])):
            s1[plane(p * 4 + g, 16), :] = x
    pl.semaphore_wait(barrier, n - 1)
    send(s1, r1, 0, WITH_LEVELS)
    send(st, rt, 1, LOW)

    tables[2] = left_weights(turn_table(n, device_turns(0)))
    tables[3] = left_weights(turn_table(n, device_turns(1)))
    tables[4] = left_weights(turn_table(n, lane_turns(1)))

    arrive(r1, 0, WITH_LEVELS)
    for p in range(2):
        x = jnp.concatenate([r1[plane(p * 4 + g, 16), :] for g in range(4)], 1)
        x = times_left(tables[2], x)
        for g, x in enumerate(columns(x)):
            half[p, g] = x
    turned = [[], []]
    for g in range(4):
        re, im = half[0, g], half[1, g]
        c, s = cos_sin(diag[1:2, :] * r1[plane(8 + g, 16), :])
        turned[0].append(re * c + im * s)
        turned[1].append(im * c - re * s)
    for p in range(2):
        x = times_left(tables[3], jnp.concatenate(turned[p], 1))
        x = times_left_turned(tables[4], jnp.concatenate(columns(x), 0))
        for g, x in enumerate(mix_blocks(columns(x), angle[1][OUTER])):
            s2[plane((g % 2) * 4 + p * 2 + g // 2), :] = x
    send(s2, r2, 2, LOW)
    send(s2, r2, 3, HIGH)

    tables[5] = left_weights(turn_table(n, row_turns(1)))
    tables[6] = left_weights(turn_table(n, row_turns(2)))
    tables[7] = left_weights(turn_table(n, device_turns(2)))
    tables[8] = left_weights(turn_table(n, lane_turns(2)))

    lane1 = lax.broadcasted_iota(jnp.int32, (1, n), 1)
    own = jnp.sum(jnp.where(lane1 == me, diag[2:3, :], 0.0), axis=1, keepdims=True)
    arrive(rt, 1, LOW)
    for g in range(4):
        c, s = cos_sin(own * rt[plane(g), :].T)
        cs[0, g] = c
        cs[1, g] = s

    for q, part in enumerate((LOW, HIGH)):
        arrive(r2, 2 + q, part)
        pair = []
        for p in range(2):
            x = jnp.concatenate([r2[plane(q * 4 + p * 2 + g), :] for g in range(2)], 1)
            pair.append(columns(times_left(tables[5], x)))
        turned = [[], []]
        for g in range(2):
            re, im = pair[0][g], pair[1][g]
            c, s = cs[0, g * 2 + q], cs[1, g * 2 + q]
            turned[0].append(re * c + im * s)
            turned[1].append(im * c - re * s)
        for p in range(2):
            x = times_left(tables[6], jnp.concatenate(turned[p], 1))
            x = times_left_turned(tables[7], jnp.concatenate(columns(x), 0))
            for g, x in enumerate(mix_pair(*columns(x), angle[2][OUTER])):
                s3[plane(q * 4 + p * 2 + g), :] = x
        send(s3, r3, 4 + q, part, (each_peer, each_peer_by_plane)[q])

    for q, part in enumerate((LOW, HIGH)):
        arrive(r3, 4 + q, part)
        for p in range(2):
            x = jnp.concatenate([r3[plane(q * 4 + p * 2 + g), :] for g in range(2)], 1)
            for g, x in enumerate(columns(times_left(tables[8], x))):
                half[p, g * 2 + q] = x.T
    for h in range(2):
        pairs = [mix_pair(half[p, h * 2], half[p, h * 2 + 1], angle[2][OUTER]) for p in range(2)]
        for q in range(2):
            re, im = pairs[0][q], pairs[1][q]
            pr, pi = power(h * 2 + q)
            out[0, h * 2 + q] = re * pr + im * pi
            out[1, h * 2 + q] = im * pr - re * pi

    sent(s1, 0, WITH_LEVELS)
    sent(st, 1, LOW)
    for q, part in enumerate((LOW, HIGH)):
        sent(s2, 2 + q, part)
        sent(s3, 4 + q, part)


def fused(wave_parts, level_table, diagonal_angles, turn_angles, na, nb):
    n = na * nb
    f32 = jnp.float32
    V = pltpu.VMEM
    tiles, tall = V((n * 8, n), f32), V((n * 16, n), f32)
    inputs = [
        pltpu.with_memory_space_constraint(x, pltpu.HBM)
        for x in (wave_parts, level_table, diagonal_angles, turn_angles)
    ]
    return pl.pallas_call(
        functools.partial(kernel, na, nb),
        out_shape=jax.ShapeDtypeStruct(wave_parts.shape, f32),
        in_specs=[pl.BlockSpec(memory_space=pltpu.HBM)] * 4,
        out_specs=pl.BlockSpec(memory_space=pltpu.VMEM),
        scratch_shapes=[
            V(wave_parts.shape, f32), V(level_table.shape, f32), V(diagonal_angles.shape, f32),
            pltpu.SMEM(turn_angles.shape, f32), pltpu.SemaphoreType.DMA((4,)),
            tiles, tiles, tall, tall, tiles, tiles, tiles, tiles,
            V((2,) + level_table.shape, f32), V(wave_parts.shape, f32),
            V((9, 2 * n, 2 * n), jnp.bfloat16),
            pltpu.SemaphoreType.DMA((6,)), pltpu.SemaphoreType.DMA((6,)),
        ],
        compiler_params=pltpu.CompilerParams(
            collective_id=0, has_side_effects=True, vmem_limit_bytes=32 * 1024 * 1024),
    )(*inputs)


def solution(mesh):
    na, nb = mesh.shape["qa"], mesh.shape["qb"]

    def each(wave_parts, level_table, diagonal_angles, turn_angles):
        return fused(wave_parts, level_table, diagonal_angles, turn_angles, na, nb)

    placed = (
        P("trial", ("qa", "qb"), None, None),
        P(("trial", "qa", "qb"), None, None),
        P("trial", None),
        P("trial", None),
    )
    return jax.shard_map(
        each,
        mesh=mesh,
        in_specs=placed,
        out_specs=P("trial", ("qa", "qb"), None, None),
        check_vma=False,
    )
```
